32 devices in a mesh: section: 4 (over x, core), tensor: 8 (over z, y).
Axes of the slice: x: 2, y: 2, z: 4, core: 2. Of those that a mesh axis runs over, the one named last changes fastest.
Arguments:
- tokens: bfloat16 [2, 64, 4096], replicated, may hold values from -6 to 6
- norm_gain: bfloat16 [4, 4096], replicated, may hold values from 0.25 to 1.75
- w_in: bfloat16 [4, 2, 14336, 4096], P('section', None, 'tensor'), may hold values from -0.09375 to 0.09375
- w_out: bfloat16 [4, 14336, 4096], P('section', 'tensor'), may hold values from -0.046875 to 0.046875
- backup_in: bfloat16 [4, 2, 14336, 4096], P('section', None, 'tensor'), may hold values from -0.09375 to 0.09375
- backup_out: bfloat16 [4, 14336, 4096], P('section', None, 'tensor'), may hold values from -0.046875 to 0.046875
- layer_group: int32 [4], replicated, may hold values from 0 to 3, as said below
- token_counts: int32 [2], replicated, may hold values from 1 to 64, as said below
Outputs:
- handed: bfloat16 [4, 2, 64, 4096], P('section', None, 'tensor')
The draws below stay inside these ranges and needn't reach their ends.
Inputs may be any that keep to these rules, and one draw needn't show every extreme that they name: layer_group[l] is l or l + 1. The layers that move up form one run of consecutive layers, at least one, that starts at the layer of the one group left without any layer; that group is never the last one. `token_counts`: rows of a micro-batch from its count on are padding. One micro-batch is full, with 64 real tokens; the other has at most 32.
All inputs are finite; a program needn't handle non-finite values.
Results may differ from the reference program's by a relative error of at most 0.025.
Values may be sent and summed in bfloat16 or wider, within the bound.
A program may use at most 192 MiB of HBM per device.

```python
import jax
import jax.numpy as jnp
from jax import lax

D = 4096
FF = 14336
TOK = 64
MB = 2
LAYERS = 4
BLOCKS = 8


def draw_layer_group(key, part):
    key_lost, key_span = jax.random.split(jax.random.fold_in(key, 7))
    lost_group = jax.random.randint(key_lost, (), 0, LAYERS - 1)
    span_count = 1 + jax.random.randint(key_span, (), 0, LAYERS - 1 - lost_group)
    levels = jnp.arange(LAYERS, dtype=jnp.int32)
    moved_up = (levels >= lost_group) & (levels < lost_group + span_count)
    return levels + moved_up.astype(jnp.int32)


def draw_token_counts(key, part):
    key_low, key_flip = jax.random.split(jax.random.fold_in(key, 11))
    high_count = jnp.int32(TOK)
    low_count = jax.random.randint(key_low, (), 1, TOK // 2 + 1)
    flipped = jax.random.randint(key_flip, (), 0, 2)
    first = jnp.where(flipped == 1, low_count, high_count)
    second = jnp.where(flipped == 1, high_count, low_count)
    return jnp.stack([first, second]).astype(jnp.int32)


def block_levels(key, shape, cuts, smallest, high):
    gain, own = 1.0, jax.random.fold_in(key, 6)
    for dim, parts in cuts:
        steps = jnp.exp(jax.random.uniform(jax.random.fold_in(own, dim), (parts,), jnp.float32, smallest / len(cuts), high / len(cuts)))
        gain = gain * jnp.repeat(steps, shape[dim] // parts).reshape([-1 if axis == dim else 1 for axis in range(len(shape))])
    return gain


def gaussian(stream_key, extent, scale, reach, cuts=(), kind=jnp.bfloat16):
    result = jax.random.normal(stream_key, extent, jnp.float32) * scale
    if len(cuts) > 0:
        result = block_levels(stream_key, extent, cuts, -0.22, 0.18) * result
    return jnp.clip(result, min=-reach, max=reach).astype(kind)


def setup_inputs(seed: int = 0) -> dict:
    splits = jax.random.split(jax.random.key(seed), 9)
    tokens = gaussian(splits[0], (MB, TOK, D), 1.0, 6.0)
    norm_gain = jnp.clip(1.0 + 0.15 * jax.random.normal(splits[1], (LAYERS, D), jnp.float32), 0.25, 1.75).astype(jnp.bfloat16)
    w_in = gaussian(splits[2], (LAYERS, 2, FF, D), D ** -0.5, 0.09375, ((0, 4), (2, 8)))
    w_out = gaussian(splits[3], (LAYERS, FF, D), FF ** -0.5, 0.046875, ((0, 4), (1, 8)))
    backup_in = gaussian(splits[4], (LAYERS, 2, FF, D), D ** -0.5, 0.09375, ((0, 4), (2, 8)))
    backup_out = gaussian(splits[5], (LAYERS, FF, D), FF ** -0.5, 0.046875, ((0, 4), (2, 8)))
    layer_group = draw_layer_group(jax.random.fold_in(splits[8], 71), 0)
    token_counts = draw_token_counts(jax.random.fold_in(splits[8], 71), 0)
    return {"tokens": tokens, "norm_gain": norm_gain, "w_in": w_in, "w_out": w_out, "backup_in": backup_in, "backup_out": backup_out, "layer_group": layer_group, "token_counts": token_counts}


NORM_EPS = 0.25

def apply_layer(current, gain_row, w_pair, w_down, row_keep):
    wide_x = current.astype(jnp.float32)
    mean_square = lax.optimization_barrier(jnp.mean(wide_x * wide_x, axis=1, keepdims=True))
    normed = (wide_x * lax.rsqrt(mean_square + NORM_EPS) * gain_row.astype(jnp.float32)).astype(jnp.bfloat16)
    gate_part = lax.dot_general(normed, w_pair[0], (((1,), (1,)), ((), ())), preferred_element_type=jnp.float32)
    up_part = lax.dot_general(normed, w_pair[1], (((1,), (1,)), ((), ())), preferred_element_type=jnp.float32)
    hidden = (jax.nn.silu(gate_part) * up_part).astype(jnp.bfloat16)
    row_count = hidden.shape[0]
    block_width = FF // BLOCKS
    hidden_blocks = hidden.reshape(row_count, BLOCKS, block_width).astype(jnp.float32)
    down_blocks = w_down.reshape(BLOCKS, block_width, D).astype(jnp.float32)
    partial_value = jnp.einsum('rbf,bfd->brd', hidden_blocks, down_blocks)
    rounded = lax.optimization_barrier(partial_value.astype(jnp.bfloat16))
    summed = lax.optimization_barrier(jnp.sum(rounded.astype(jnp.float32), axis=0))
    return (wide_x + row_keep * summed).astype(jnp.bfloat16)

def reference(tokens, norm_gain, w_in, w_out, backup_in, backup_out, layer_group, token_counts):
    positions = jnp.arange(TOK, dtype=jnp.int32)
    row_keep = (positions[None, :] < token_counts[:, None]).astype(jnp.float32).reshape(MB * TOK, 1)
    current = tokens.reshape(MB * TOK, D)
    history = [current]
    for level in range(LAYERS):
        moved = layer_group[level] == level + 1
        spare = (level + 1) % LAYERS
        pair = jnp.where(moved, backup_in[spare], w_in[level])
        down = jnp.where(moved, backup_out[spare], w_out[level])
        current = apply_layer(current, norm_gain[level][None, :], pair, down, row_keep)
        history.append(current)
    stacked = jnp.stack(history).reshape(LAYERS + 1, MB, TOK, D)
    groups = jnp.arange(LAYERS, dtype=jnp.int32)
    reached = lax.optimization_barrier(jnp.sum((layer_group[None, :] <= groups[:, None]).astype(jnp.int32), axis=1))
    return jnp.take(stacked, reached, axis=0)
```

```python
import functools

import jax
import jax.numpy as jnp
from jax import lax
from jax.experimental import pallas as pl
from jax.experimental.pallas import tpu as pltpu
from jax.sharding import PartitionSpec as P

NORM_EPS = 0.25
MESH = pl.DeviceIdType.MESH


def exchange_kernel(n, source, groups, scatter, slotted, width, src, out, send_sem, recv_sem, local_sem):
    group = lax.axis_index("section")
    me = lax.axis_index("tensor")
    barrier = pltpu.get_barrier_semaphore()
    is_source = group == source

    def peer(offset):
        return lax.rem(me + offset, n)

    def place(position):
        if slotted:
            return out.at[position]
        return out.at[:, pl.ds(pl.multiple_of(position * width, 128), width)]

    def block(position):
        if scatter:
            return src.at[:, pl.ds(pl.multiple_of(position * width, 128), width)]
        return src

    def copy_to(index, target, offset):
        return pltpu.make_async_remote_copy(
            src_ref=block(peer(offset)),
            dst_ref=place(me),
            send_sem=send_sem.at[index * n + offset],
            recv_sem=recv_sem.at[offset],
            device_id=(target, peer(offset)),
            device_id_type=MESH,
        )

    def arrival(offset):
        origin = lax.rem(me - offset + n, n)
        return pltpu.make_async_remote_copy(
            src_ref=block(me),
            dst_ref=place(origin),
            send_sem=send_sem.at[0],
            recv_sem=recv_sem.at[offset],
            device_id=(source, origin),
            device_id_type=MESH,
        )

    sends = [
        (index, target, offset)
        for offset in range(n)
        for index, target in enumerate(groups)
        if target != source or offset > 0
    ]

    @pl.when(is_source)
    def _():
        for _, target, offset in sends:
            pl.semaphore_signal(barrier, inc=1, device_id=(target, peer(offset)), device_id_type=MESH)
        pl.semaphore_wait(barrier, len(sends))
        kept = pltpu.make_async_copy(block(me), place(me), local_sem)
        for send in sends:
            copy_to(*send).start()
        kept.start()
        kept.wait()
        for offset in range(1, n):
            arrival(offset).wait_recv()
        for send in sends:
            copy_to(*send).wait_send()

    for target in groups:
        if target != source:

            @pl.when(group == target)
            def _():
                for offset in range(n):
                    pl.semaphore_signal(
                        barrier, inc=1, device_id=(source, peer(offset)), device_id_type=MESH
                    )
                pl.semaphore_wait(barrier, n)
                for offset in range(n):
                    arrival(offset).wait_recv()


def exchange(block, n, source, groups, scatter, slotted, channel):
    rows = block.shape[0]
    width = block.shape[1] // n if scatter else block.shape[1]
    shape = (n, rows, width) if slotted else (rows, n * width)
    return pl.pallas_call(
        functools.partial(exchange_kernel, n, source, groups, scatter, slotted, width),
        out_shape=jax.ShapeDtypeStruct(shape, block.dtype),
        in_specs=[pl.BlockSpec(memory_space=pltpu.VMEM)],
        out_specs=pl.BlockSpec(memory_space=pltpu.VMEM),
        scratch_shapes=[
            pltpu.SemaphoreType.DMA((n * len(groups),)),
            pltpu.SemaphoreType.DMA((n,)),
            pltpu.SemaphoreType.DMA,
        ],
        compiler_params=pltpu.CompilerParams(collective_id=channel, has_side_effects=True),
        name=f"exchange_{channel}",
    )(block)


def project_in(current, gain_row, w_pair):
    wide_x = current.astype(jnp.float32)
    mean_square = jnp.mean(wide_x * wide_x, axis=1, keepdims=True)
    normed = (wide_x * lax.rsqrt(mean_square + NORM_EPS) * gain_row.astype(jnp.float32)).astype(
        jnp.bfloat16
    )
    gate_part = lax.dot_general(
        normed, w_pair[0], (((1,), (1,)), ((), ())), preferred_element_type=jnp.float32
    )
    up_part = lax.dot_general(
        normed, w_pair[1], (((1,), (1,)), ((), ())), preferred_element_type=jnp.float32
    )
    return (jax.nn.silu(gate_part) * up_part).astype(jnp.bfloat16)


def shards(tokens, norm_gain, w_in, w_out, backup_in, backup_out, layer_group, token_counts):
    section_id = lax.axis_index("section")
    sections = lax.axis_size("section")
    tensor_id = lax.axis_index("tensor")
    n = lax.axis_size("tensor")
    _, tok_rows, features = tokens.shape
    layers = layer_group.shape[0]
    half = tok_rows // 2
    row_share = tok_rows // n
    width = features // n
    channels = iter(range(1000))

    full_second = token_counts[1] > token_counts[0]
    full_tokens = jnp.where(full_second, tokens[1], tokens[0])
    part_tokens = jnp.where(full_second, tokens[0], tokens[1])
    part_count = jnp.minimum(token_counts[0], token_counts[1])
    current = jnp.concatenate([full_tokens, part_tokens[:half]], axis=0)
    places = jnp.arange(tok_rows + half, dtype=jnp.int32)
    keep = ((places < tok_rows) | (places - tok_rows < part_count)).astype(jnp.float32)[:, None]
    reached = jnp.sum((layer_group <= section_id).astype(jnp.int32))

    def own_columns(x):
        return lax.dynamic_slice_in_dim(x, tensor_id * width, width, 1).astype(jnp.float32)

    def moved_up(level):
        return layer_group[level] == level + 1

    def hand_on(columns, level, source):
        first = tuple(g for g in (source, level + 1) if g < sections)
        near = tuple(sorted(set(first)))
        far = tuple(sorted(set(first + ((level + 2,) if level + 2 < sections else ()))))
        if near == far or level + 1 >= layers:
            return exchange(columns, n, source, near, False, False, next(channels))
        return lax.cond(
            moved_up(level + 1),
            functools.partial(
                exchange, n=n, source=source, groups=far, scatter=False, slotted=False,
                channel=next(channels)
            ),
            functools.partial(
                exchange, n=n, source=source, groups=near, scatter=False, slotted=False,
                channel=next(channels)
            ),
            columns,
        )

    def own_layer(x, level):
        hidden = project_in(x, norm_gain[level][None], w_in[0])
        partial_value = jnp.dot(hidden, w_out[0], preferred_element_type=jnp.float32)
        arrived = exchange(
            partial_value.astype(jnp.bfloat16), n, level, (level,), True, True, next(channels)
        )
        summed = jnp.sum(arrived.astype(jnp.float32), axis=0)
        return hand_on((own_columns(x) + keep * summed).astype(jnp.bfloat16), level, level)

    def moved_layer(x, level):
        source = level + 1
        hidden = project_in(x, norm_gain[level][None], backup_in[0])
        full_hidden = exchange(hidden, n, source, (source,), False, True, next(channels))
        block_width = hidden.shape[1]
        summed = jnp.zeros((x.shape[0], width), jnp.float32)
        pieces = [
            jnp.dot(
                full_hidden[b],
                backup_out[0, b * block_width : (b + 1) * block_width],
                preferred_element_type=jnp.float32,
            ).astype(jnp.bfloat16)
            for b in range(n)
        ]
        for piece in lax.optimization_barrier(pieces):
            summed = summed + piece.astype(jnp.float32)
        return hand_on((own_columns(x) + keep * summed).astype(jnp.bfloat16), level, source)

    states = [current]
    for level in range(layers):
        if level + 1 < sections:
            current = lax.cond(
                moved_up(level),
                functools.partial(moved_layer, level=level),
                functools.partial(own_layer, level=level),
                current,
            )
        else:
            current = own_layer(current, level)
        states.append(current)

    def row_block(x, start):
        return lax.dynamic_slice_in_dim(x, start, row_share, 0)

    start = tensor_id * row_share
    full_rows = row_block(states[0], start)
    part_rows = row_block(part_tokens, start)
    in_half = start < half
    part_start = jnp.where(in_half, tok_rows + start, 0)
    for level in range(layers):
        here = reached == level + 1
        full_rows = jnp.where(here, row_block(states[level + 1], start), full_rows)
        part_rows = jnp.where(
            here & in_half, row_block(states[level + 1], part_start), part_rows
        )
    handed = jnp.stack(
        [
            jnp.where(full_second, part_rows, full_rows),
            jnp.where(full_second, full_rows, part_rows),
        ]
    )
    return handed[None]


def solution(mesh):
    return jax.shard_map(
        shards,
        mesh=mesh,
        in_specs=(
            P(),
            P(),
            P("section", None, "tensor", None),
            P("section", "tensor", None),
            P("section", None, "tensor", None),
            P("section", None, "tensor"),
            P(),
            P(),
        ),
        out_specs=P("section", None, "tensor", None),
        check_vma=False,
    )
```
